32 devices in a mesh: tile: 8 (over z, x), mem: 4 (over y, core).
Axes of the slice: x: 2, y: 2, z: 4, core: 2. Of those that a mesh axis runs over, the one named last changes fastest.
Arguments:
- ensemble: bfloat16 [64, 128, 1024], P('mem', 'tile'), may hold values from -8 to 8
- obs_members: bfloat16 [4096, 64, 128], P(('tile', 'mem')), may hold values from -6 to 6
- obs_values: float32 [4096, 128], P(('tile', 'mem')), may hold values from -9 to 9
- obs_weight: float32 [4096, 128], P(('tile', 'mem')), may hold values from 0.05 to 1
- obs_count: int32 [4096], P(('tile', 'mem')), may hold values from 1 to 128
- obs_tile: int32 [4096], P(('tile', 'mem')), may hold values from 0 to 7, as said below
- obs_block: int32 [4096], P(('tile', 'mem')), may hold values from 0 to 15
- obs_turn: int32 [4096], P(('tile', 'mem')), may hold values from 0 to 3
Outputs:
- analysis_pert: bfloat16 [64, 128, 1024], P('mem', 'tile')
- analysis_mean: bfloat16 [128, 1024], P(('tile', 'mem'))
The draws below stay inside these ranges and needn't reach their ends.
Inputs may be any that keep to these rules, and one draw needn't show every extreme that they name: `obs_tile`: within each aligned group of 128 consecutive blocks (the blocks of one device), no tile is named more than 32 times, and one tile is named exactly 32 times by every group.
All inputs are finite; a program needn't handle non-finite values.
Results may differ from the reference program's by a relative error of at most 0.0036.
Values may be sent and summed in bfloat16 or wider, within the bound.
No kernel may reach another device: no remote copies, remote signals or barrier semaphores. Data moves between devices by JAX's collectives and lax.ppermute only.
A program may use at most 64 MiB of HBM per device.

```python
import math
import jax
import jax.numpy as jnp
from jax import lax

MEMBERS = 64
BPS = 4
ROWS = 128
OBD = 128
NS_STEPS = 6
ABLK = 16
LEVBC = 1024
NBLK = 128
NOB = 4096
N_TILE = 8


def draw_ensemble(key, part):
    centre_key = jax.random.fold_in(key, 11)
    member_key = jax.random.fold_in(key, 12)
    centre = jax.random.normal(centre_key, (NBLK, LEVBC), jnp.float32)
    members = 0.7 * jax.random.normal(member_key, (MEMBERS, NBLK, LEVBC), jnp.float32)
    return jnp.clip(centre[None] + members, -8.0, 8.0).astype(jnp.bfloat16)


def draw_obs_tile(key, part):
    capacity = max(2, 2 * OBD // N_TILE)
    slot_count = N_TILE * capacity
    liking = jax.random.randint(jax.random.fold_in(key, 21), (N_TILE,), 0, 4)
    hottest = jax.random.randint(jax.random.fold_in(key, 22), (), 0, N_TILE)
    slot_tile = jnp.arange(slot_count, dtype=jnp.int32) // capacity
    favour = liking[slot_tile] * 32768 + jnp.where(slot_tile == hottest, 1048576, 0)

    def one_source(source):
        source_key = jax.random.fold_in(jax.random.fold_in(key, 23), source)
        jitter = jax.random.randint(source_key, (slot_count,), 0, 65536)
        scores = (jitter + favour) * slot_count + jnp.arange(slot_count, dtype=jnp.int32)
        _, picked = lax.top_k(scores, OBD)
        shuffle = jax.random.permutation(jax.random.fold_in(source_key, 1), OBD)
        return (picked // capacity)[shuffle].astype(jnp.int32)
    sources = jnp.arange(NOB // OBD, dtype=jnp.int32)
    return jax.vmap(one_source)(sources).reshape(NOB)


def with_ends(array, rng, low, largest):
    shape = array.shape
    spot = [jax.random.randint(jax.random.fold_in(rng, axis), (), 0, shape[axis]) for axis in range(len(shape))]
    array = array.at[tuple(spot)].set(low)
    longest = shape.index(max(shape))
    spot[longest] = (spot[longest] + 1) % shape[longest]
    return array.at[tuple(spot)].set(largest)


def block_levels(stream_key, dims, cuts, least, high):
    def one(dim, shards_of):
        steps = jax.random.uniform(jax.random.fold_in(jax.random.fold_in(stream_key, 6), dim), (shards_of,), jnp.float32, least / len(cuts), high / len(cuts))
        return jnp.repeat(jnp.exp(steps), dims[dim] // shards_of).reshape((-1,) + (1,) * (len(dims) - dim - 1))

    loudness = one(*cuts[0])
    for cut in cuts[1:]:
        loudness = loudness * one(*cut)
    return loudness


def bell_draw(key, extent, scale, limit, shards=(), held_as=jnp.bfloat16):
    values = scale * jax.random.normal(key, extent, jnp.float32)
    if shards:
        values = values * block_levels(key, extent, shards, -0.22, 0.18)
    return jnp.clip(values, -limit, limit).astype(held_as)


def setup_inputs(seed: int = 0) -> dict:
    keys = jax.random.split(jax.random.key(seed), 9)
    ensemble = draw_ensemble(jax.random.fold_in(keys[8], 71), 0)
    obs_members = bell_draw(keys[1], (NOB, MEMBERS, ROWS), 1.0, 6.0, ((0, 32),))
    obs_values = bell_draw(keys[2], (NOB, ROWS), 1.5, 9.0, ((0, 32),), jnp.float32)
    obs_weight = jnp.clip(jnp.exp(math.log(1.0) - 2.9957323 * jax.random.uniform(keys[3], (NOB, ROWS), jnp.float32) ** block_levels(keys[3], (NOB, ROWS), ((0, 32),), -0.2, 0.2)), 0.05, 1.0)
    obs_count = with_ends(jax.random.randint(keys[4], (NOB,), 1, ROWS + 1), jax.random.fold_in(keys[4], 1), 1, ROWS).astype(jnp.int32)
    obs_tile = draw_obs_tile(jax.random.fold_in(keys[8], 71), 0)
    obs_block = with_ends(jax.random.randint(keys[6], (NOB,), 0, ABLK), jax.random.fold_in(keys[6], 1), 0, ABLK - 1).astype(jnp.int32)
    obs_turn = with_ends(jax.random.randint(keys[7], (NOB,), 0, 4), jax.random.fold_in(keys[7], 1), 0, 3).astype(jnp.int32)
    return {"ensemble": ensemble, "obs_members": obs_members, "obs_values": obs_values, "obs_weight": obs_weight, "obs_count": obs_count, "obs_tile": obs_tile, "obs_block": obs_block, "obs_turn": obs_turn}


def product(left, right):
    return jnp.matmul(left, right, precision=lax.Precision.HIGHEST)

def target_block(obs_block, obs_turn):
    block_row = obs_block // BPS
    block_col = obs_block % BPS
    last = BPS - 1
    new_row = jnp.where(obs_turn == 0, block_row, jnp.where(obs_turn == 1, block_col, jnp.where(obs_turn == 2, last - block_row, last - block_col)))
    new_col = jnp.where(obs_turn == 0, block_col, jnp.where(obs_turn == 1, last - block_row, jnp.where(obs_turn == 2, last - block_col, block_row)))
    return (new_row * BPS + new_col).astype(jnp.int32)

def scaled_obs(obs_members, obs_values, obs_weight, obs_count):
    obs_mean = lax.optimization_barrier(jnp.sum(obs_members.astype(jnp.float32), axis=1)) / MEMBERS
    usable = lax.broadcasted_iota(jnp.int32, obs_weight.shape, 1) < obs_count[:, None]
    weight_root = jnp.sqrt(jnp.where(usable, obs_weight, jnp.zeros_like(obs_weight)))
    scaled_pert = ((obs_members.astype(jnp.float32) - obs_mean[:, None, :]) * weight_root[:, None, :]).astype(jnp.bfloat16)
    scaled_innov = ((obs_values - obs_mean) * weight_root).astype(jnp.bfloat16)
    return (scaled_pert, scaled_innov)

def transforms(gram, projection):
    identity = jnp.eye(MEMBERS, dtype=jnp.float32)
    system = (MEMBERS - 1.0) * identity + gram
    frob = jnp.sqrt(lax.optimization_barrier(jnp.sum(system * system, axis=(1, 2))))[:, None, None]
    square_root = system / frob
    inverse = jnp.broadcast_to(identity, system.shape)
    for sweep in range(NS_STEPS):
        middle = 1.5 * identity - 0.5 * product(inverse, square_root)
        square_root = product(square_root, middle)
        inverse = product(middle, inverse)
    inverse_root = inverse / jnp.sqrt(frob)
    covariance = product(inverse_root, inverse_root)
    mean_weights = jnp.einsum('bjk,bk->bj', covariance, projection, precision=lax.Precision.HIGHEST).astype(jnp.bfloat16)
    spread = (jnp.sqrt(MEMBERS - 1.0) * inverse_root).astype(jnp.bfloat16)
    return (spread, mean_weights)

def reference(ensemble, obs_members, obs_values, obs_weight, obs_count, obs_tile, obs_block, obs_turn):
    scaled_pert, scaled_innov = scaled_obs(obs_members, obs_values, obs_weight, obs_count)
    segment = (obs_tile * ABLK + target_block(obs_block, obs_turn)).astype(jnp.int32)
    groups = NOB // OBD

    def add_group(carry, pieces):
        gram_total, proj_total = carry
        pert_piece, innov_piece, seg_piece = pieces
        pert_float = pert_piece.astype(jnp.float32)
        innov_float = innov_piece.astype(jnp.float32)
        grams = jnp.einsum('nkr,nlr->nkl', pert_float, pert_float, precision=lax.Precision.HIGHEST)
        projs = jnp.einsum('nkr,nr->nk', pert_float, innov_float, precision=lax.Precision.HIGHEST)
        return ((gram_total.at[seg_piece].add(grams), proj_total.at[seg_piece].add(projs)), None)
    start = (jnp.zeros((NBLK, MEMBERS, MEMBERS), jnp.float32), jnp.zeros((NBLK, MEMBERS), jnp.float32))
    pieces = (scaled_pert.reshape(groups, OBD, MEMBERS, ROWS), scaled_innov.reshape(groups, OBD, ROWS), segment.reshape(groups, OBD))
    (gram, projection), _ = lax.scan(add_group, start, pieces)
    spread, mean_weights = transforms(gram, projection)
    background_mean = lax.optimization_barrier(jnp.sum(ensemble.astype(jnp.float32), axis=0)) / MEMBERS
    perturbation = (ensemble.astype(jnp.float32) - background_mean[None]).astype(jnp.bfloat16)
    pert_float = perturbation.astype(jnp.float32)
    analysis_pert = jnp.einsum('jbx,bjk->kbx', pert_float, spread.astype(jnp.float32), precision=lax.Precision.HIGHEST).astype(jnp.bfloat16)
    increment = jnp.einsum('jbx,bj->bx', pert_float, mean_weights.astype(jnp.float32), precision=lax.Precision.HIGHEST)
    analysis_mean = (background_mean + increment).astype(jnp.bfloat16)
    return (analysis_pert, analysis_mean)
```

```python
import functools

import jax
import jax.numpy as jnp
from jax import lax
from jax.experimental import pallas as pl
from jax.experimental.pallas import tpu as pltpu
from jax.sharding import Mesh, PartitionSpec as P

BPS = 4
ABLK = BPS * BPS
NS_STEPS = 6
CORES = 2
LANES = 128
F32 = jnp.float32
BF16 = jnp.bfloat16


def iota(shape, dim):
    return lax.broadcasted_iota(jnp.int32, shape, dim)


def packed_rows(own):
    return (16 * own + own + 7) // 8 * 8


def whole(shape=None):
    return pl.BlockSpec(memory_space=pltpu.VMEM)


def scalars():
    return pl.BlockSpec(memory_space=pltpu.SMEM)


def target_of(tile, block, turn):
    row, col = block // BPS, block % BPS
    last = BPS - 1
    new_row = jnp.where(
        turn == 0, row, jnp.where(turn == 1, col, jnp.where(turn == 2, last - row, last - col))
    )
    new_col = jnp.where(
        turn == 0, col, jnp.where(turn == 1, last - row, jnp.where(turn == 2, last - col, row))
    )
    return tile * ABLK + new_row * BPS + new_col


def gram_kernel(
    own, chunks, count, tile, block, turn, values, weight, members_hbm, send, keep, members, total, sems
):
    blocks, size, rows = members.shape
    per_chunk = blocks // chunks
    copies = [
        pltpu.make_async_copy(
            members_hbm.at[pl.ds(c * per_chunk, per_chunk)],
            members.at[pl.ds(c * per_chunk, per_chunk)],
            sems.at[c],
        )
        for c in range(chunks)
    ]
    for copy in copies:
        copy.start()

    def clear(t, _):
        total[t] = jnp.zeros(total.shape[1:], F32)
        return 0

    lax.fori_loop(0, total.shape[0], clear, 0, unroll=4)
    lane = iota((1, rows), 1)
    first = iota((16, rows), 0) == 0

    def add_block(n, _):
        perts = members[n].astype(F32)
        mean = jnp.sum(perts, axis=0, keepdims=True) / size
        root = jnp.sqrt(jnp.where(lane < count[n], weight[pl.ds(n, 1), :], 0.0))
        scaled = ((perts - mean) * root).astype(BF16)
        innov = (values[pl.ds(n, 1), :] - mean) * root
        tail = jnp.where(first, innov, 0.0).astype(BF16)
        left = jnp.concatenate([scaled, tail], axis=0)
        right = jnp.concatenate([scaled, scaled], axis=0)
        products = lax.dot_general(
            left, right, (((1,), (1,)), ((), ())), preferred_element_type=F32
        )
        t = target_of(tile[n], block[n], turn[n])
        total[t] = total[t] + products[: size + 8]
        return 0

    for c in range(chunks):
        copies[c].wait()
        lax.fori_loop(c * per_chunk, (c + 1) * per_chunk, add_block, 0, unroll=4)

    half = size // 2
    lane_half = iota((half, LANES), 1)
    col = lane_half % size
    row = iota((half, LANES), 0)
    from_top = (col >= half) | (col <= row)
    on_diag = col == row
    first_of_pair = iota((size + 8, LANES), 1) < size
    core = lax.axis_index("core")
    tail_row = iota((8, LANES), 0)

    def pack(d, side):
        base = d * (CORES * own) + side * own
        bodies = []
        tail = jnp.zeros((8, LANES), F32)
        for pair in range(own // 2):
            both = jnp.where(first_of_pair, total[base + 2 * pair], total[base + 2 * pair + 1])
            top = both[:half]
            bottom = pltpu.roll(both[half:size], LANES - half, 1)
            bodies.append(jnp.where(from_top, top, bottom))
            diag = jnp.sum(jnp.where(on_diag, bottom, 0.0), axis=0, keepdims=True)
            tail = jnp.where(tail_row == 2 * pair, both[size : size + 1], tail)
            tail = jnp.where(tail_row == 2 * pair + 1, diag, tail)
        return jnp.concatenate(bodies + [tail], axis=0)

    def pack_both(d, _):
        keep[d] = pack(d, core)
        send[d] = pack(d, 1 - core).astype(BF16)
        return 0

    lax.fori_loop(0, send.shape[0], pack_both, 0)


def scaled_grams(own, count, tile, block, turn, values, weight, members, tiles):
    blocks, size, rows = members.shape
    dests = tiles * ABLK // (CORES * own)
    shape = (dests, packed_rows(own), LANES)
    chunks = 4
    return pl.pallas_call(
        functools.partial(gram_kernel, own, chunks),
        out_shape=(jax.ShapeDtypeStruct(shape, BF16), jax.ShapeDtypeStruct(shape, F32)),
        in_specs=[scalars()] * 4 + [whole(), whole(), pl.BlockSpec(memory_space=pl.ANY)],
        out_specs=(whole(), whole()),
        scratch_shapes=[
            pltpu.VMEM((blocks, size, rows), BF16),
            pltpu.VMEM((tiles * ABLK, size + 8, LANES), F32),
            pltpu.SemaphoreType.DMA((chunks,)),
        ],
        compiler_params=pltpu.CompilerParams(vmem_limit_bytes=48 * 1024 * 1024),
        name="grams",
    )(count, tile, block, turn, values, weight, members)


def split(x):
    high = x.astype(BF16)
    return high, (x - high.astype(F32)).astype(BF16)


def left_of(x, first_half):
    high, low = split(x)
    return jnp.concatenate([high, jnp.where(first_half, low, jnp.zeros_like(low))], axis=1)


def right_of(x):
    high, low = split(x)
    return jnp.concatenate([high, low, high, high], axis=0)


def times(left, right):
    return jnp.dot(left, right, preferred_element_type=F32)


def transform_kernel(own, size, groups, arrived, weights_out, *rest):
    outs, spread = rest[:groups], rest[groups]
    summed = arrived[0].astype(F32)
    for s in range(1, arrived.shape[0]):
        summed = summed + arrived[s].astype(F32)
    half = size // 2
    col = iota((half, LANES), 1) % size
    row = iota((half, LANES), 0)
    upper = col >= half
    eye = (iota((size, LANES), 1) % size == iota((size, LANES), 0)).astype(F32)
    first_half = iota((size, LANES), 1) < size
    extra = 16 * own
    systems, projections = [], []
    for pair in range(own // 2):
        part = summed[half * pair : half * (pair + 1)]
        projection = summed[extra + 2 * pair : extra + 2 * pair + 1]
        diag = pltpu.roll(summed[extra : extra + 8], half, 1)[2 * pair + 1 : 2 * pair + 2]
        low = jnp.where(col < row, part, jnp.where(col == row, 0.5 * part, 0.0))
        top = jnp.where(upper, part, low)
        moved = pltpu.roll(part, half, 1)
        high = jnp.where(
            col - half > row, moved, jnp.where(col - half == row, 0.5 * diag, 0.0)
        )
        bottom = jnp.where(upper, high, 0.0)
        fold = jnp.concatenate([top, bottom], axis=0)
        turned = fold.T
        other = pltpu.roll(fold, size, 1)
        for t in range(2):
            here = turned[size * t : size * (t + 1)]
            here = jnp.concatenate([here, here], axis=1)
            one, two = (fold, other) if t == 0 else (other, fold)
            gram = jnp.where(first_half, one, two) + here
            systems.append((size - 1.0) * eye + gram)
            shifted = projection if t == 0 else pltpu.roll(
                jnp.broadcast_to(projection, (8, LANES)), size, 1
            )[:1]
            projections.append(shifted)
    inverse_frobs, roots, inverses = [], [], []
    for system in systems:
        squares = jnp.where(first_half, system * system, 0.0)
        frob = jnp.sqrt(jnp.sum(jnp.sum(squares, axis=0, keepdims=True), axis=1, keepdims=True))
        inverse_frobs.append(frob)
        roots.append(system / frob)
    for step in range(NS_STEPS):
        if step == 0:
            middles = [1.5 * eye - 0.5 * s for s in roots]
        else:
            middles = [
                1.5 * eye - 0.5 * times(left_of(z, first_half), right_of(s))
                for z, s in zip(inverses, roots)
            ]
        if step == 0:
            roots = [times(left_of(s, first_half), right_of(e)) for s, e in zip(roots, middles)]
            inverses = middles
        elif step < NS_STEPS - 1:
            stacked = [
                times(
                    jnp.concatenate([left_of(s, first_half), left_of(z, first_half)], axis=0),
                    right_of(e),
                )
                for s, z, e in zip(roots, inverses, middles)
            ]
            roots = [x[:size] for x in stacked]
            inverses = [x[size:] for x in stacked]
        else:
            inverses = [
                times(left_of(z, first_half), right_of(e)) for z, e in zip(inverses, middles)
            ]
    share = size // groups
    me = lax.axis_index("y") * CORES + lax.axis_index("core")
    rows8 = iota((8, LANES), 0)
    weights = jnp.zeros((8, LANES), F32)
    for q in range(own):
        inverse_root = inverses[q] / jnp.sqrt(inverse_frobs[q])
        spread[q] = jnp.sqrt(size - 1.0) * inverse_root
        moved = jnp.sum(
            jnp.where(first_half, inverse_root * projections[q], 0.0), axis=1, keepdims=True
        )
        mean_weights = jnp.sum(inverse_root * moved, axis=0, keepdims=True)
        weights = jnp.where(rows8 == q, mean_weights, weights)
    weights_out[...] = weights
    for b in range(groups):
        start = pl.multiple_of((me ^ b) * share, share)
        for q in range(own):
            outs[b][pl.ds(q * share, share), :] = spread[q, pl.ds(start, share), :].astype(BF16)


def transforms(own, size, groups, arrived):
    share = size // groups
    return pl.pallas_call(
        functools.partial(transform_kernel, own, size, groups),
        out_shape=(jax.ShapeDtypeStruct((8, LANES), F32),)
        + tuple(jax.ShapeDtypeStruct((own * share, LANES), BF16) for _ in range(groups)),
        in_specs=[whole()],
        out_specs=tuple([whole()] * (groups + 1)),
        scratch_shapes=[pltpu.VMEM((own, size, LANES), F32)],
        name="transforms",
    )(arrived)


def centre_kernel(own, *refs):
    groups = len(refs) - 2
    parts, pert, mean_out = refs[:groups], refs[groups], refs[groups + 1]
    share, ablk, width = parts[0].shape
    me = lax.axis_index("y") * CORES + lax.axis_index("core")
    size = share * groups
    step = 256

    def one(c, _):
        at = pl.ds(pl.multiple_of(c * step, step), step)
        total = jnp.zeros((ablk, step), F32)
        for part in parts:
            for i in range(share):
                total = total + part[i, :, at].astype(F32)
        mean = total / size
        mean_out[:, at] = mean
        for b, part in enumerate(parts):
            for i in range(share):
                pert[pl.ds((b * share + i) * ablk, ablk), at] = (
                    part[i, :, at].astype(F32) - mean
                ).astype(BF16)
        return 0

    lax.fori_loop(0, width // step, one, 0)


def centred(own, parts):
    share, ablk, width = parts[0].shape
    return pl.pallas_call(
        functools.partial(centre_kernel, own),
        out_shape=(
            jax.ShapeDtypeStruct((len(parts) * share * ablk, width), BF16),
            jax.ShapeDtypeStruct((ablk, width), F32),
        ),
        in_specs=[whole()] * len(parts),
        out_specs=(whole(), whole()),
        name="centre",
    )(*parts)


def apply_kernel(own, groups, weights, pert, mean, *refs):
    arrived, out_pert, out_mean = refs[:groups], refs[groups], refs[groups + 1]
    size_by_block, width = pert.shape
    share = arrived[0].shape[0] // own
    rows = share * ABLK
    me = lax.axis_index("y") * CORES + lax.axis_index("core")
    received = jnp.concatenate([r[...] for r in arrived], axis=0)
    per_source = own * share
    count = groups * per_source
    to_row = iota((rows, count), 0)
    from_row = iota((rows, count), 1)
    source = me ^ (from_row // per_source)
    within = from_row % per_source
    place = (to_row // ABLK == within % share) & (
        to_row % ABLK == source * own + within // share
    )
    spread = times(place.astype(F32).astype(BF16), received).astype(BF16)
    spread = jnp.concatenate([spread, weights[...].astype(BF16), jnp.zeros((8, LANES), BF16)], axis=0)
    column = iota((LANES, size_by_block), 1)
    member = (me ^ (column // (share * ABLK))) * share + (column // ABLK) % share
    repeat = (iota((LANES, size_by_block), 0) == member).astype(F32).astype(BF16)
    wide = times(spread, repeat)
    wide_row = iota(wide.shape, 0)
    block = jnp.where(wide_row < rows, wide_row % ABLK, me * own + wide_row - rows)
    wide = jnp.where(block == iota(wide.shape, 1) % ABLK, wide, 0.0).astype(BF16)
    step = 256
    for c in range(width // step):
        at = pl.ds(c * step, step)
        result = times(wide, pert[:, at])
        out_pert[:, at] = result[:rows].astype(BF16)
        means = mean[:, at]
        own_mean = means[:own]
        for m in range(1, groups):
            own_mean = jnp.where(me == m, means[m * own : (m + 1) * own], own_mean)
        out_mean[:, at] = (own_mean + result[rows : rows + own]).astype(BF16)


def applied(own, weights, pert, mean, arrived):
    groups = len(arrived)
    share = arrived[0].shape[0] // own
    width = pert.shape[1]
    return pl.pallas_call(
        functools.partial(apply_kernel, own, groups),
        out_shape=(
            jax.ShapeDtypeStruct((share * ABLK, width), BF16),
            jax.ShapeDtypeStruct((own, width), BF16),
        ),
        in_specs=[whole()] * (3 + groups),
        out_specs=(whole(), whole()),
        name="apply",
    )(weights, pert, mean, *arrived)


def body(ensemble, obs_members, obs_values, obs_weight, obs_count, obs_tile, obs_block, obs_turn):
    tiles = lax.axis_size("tile")
    rows_y = lax.axis_size("y")
    groups = rows_y * CORES
    own = ABLK // groups
    size = obs_members.shape[1]
    across = [(i, i ^ 1) for i in range(CORES)]

    def swapped(x, b):
        pairs = [(i, i ^ b) for i in range(groups)]
        return lax.ppermute(x, ("y", "core"), pairs)

    parts = [ensemble, swapped(ensemble, 1)]
    for b in range(2, groups, 2):
        far = swapped(ensemble, b)
        parts += [far, lax.ppermute(far, "core", across)]
    send, keep = scaled_grams(
        own, obs_count, obs_tile, obs_block, obs_turn, obs_values, obs_weight, obs_members, tiles
    )
    got = lax.ppermute(send, "core", across)
    mine = (keep + got.astype(F32)).astype(BF16)
    arrived = lax.all_to_all(mine, ("tile", "y"), split_axis=0, concat_axis=0, tiled=True)
    pert, mean = centred(own, parts)
    weights, *spreads = transforms(own, size, groups, arrived)
    spreads = [spreads[0]] + [swapped(s, b) for b, s in enumerate(spreads) if b]
    analysis_pert, analysis_mean = applied(own, weights, pert, mean, spreads)
    return analysis_pert.reshape(ensemble.shape), analysis_mean


def solution(mesh):
    tiles, groups = mesh.shape["tile"], mesh.shape["mem"]
    fine = Mesh(mesh.devices.reshape(tiles, groups // CORES, CORES), ("tile", "y", "core"))
    everyone = ("tile", "y", "core")
    placed = (
        P(("y", "core"), "tile", None),
        P(everyone, None, None),
        P(everyone, None),
        P(everyone, None),
        P(everyone),
        P(everyone),
        P(everyone),
        P(everyone),
    )
    return jax.shard_map(
        body,
        mesh=fine,
        in_specs=placed,
        out_specs=(P(("y", "core"), "tile", None), P(everyone, None)),
        check_vma=False,
    )
```

```python
import functools

import jax
import jax.numpy as jnp
from jax import lax
from jax.experimental import pallas as pl
from jax.experimental.pallas import tpu as pltpu
from jax.sharding import Mesh, PartitionSpec as P


BPS = 4
ABLK = BPS * BPS
NS_STEPS = 6
CORES = 2
LANES = 128
F32 = jnp.float32
BF16 = jnp.bfloat16


def iota(shape, dim):
    return lax.broadcasted_iota(jnp.int32, shape, dim)


def packed_rows(own):
    return (16 * own + own + 7) // 8 * 8


def whole():
    return pl.BlockSpec(memory_space=pltpu.VMEM)


def target_of(tile, block, turn):
    row, col = block >> 2, block & 3
    last = BPS - 1
    new_row = jnp.where(
        turn == 0, row, jnp.where(turn == 1, col, jnp.where(turn == 2, last - row, last - col))
    )
    new_col = jnp.where(
        turn == 0, col, jnp.where(turn == 1, last - row, jnp.where(turn == 2, last - col, row))
    )
    return tile * ABLK + new_row * BPS + new_col


def gram_kernel(own, chunks, *refs):
    sources, (send, keep) = refs[:7], refs[7:9]
    held, total, sems = refs[9:16], refs[16], refs[17]
    count, tile, block, turn, values, weight, members = held
    blocks, size, rows = members.shape
    per_chunk = blocks // chunks

    def fetch(c):
        at = pl.ds(pl.multiple_of(c * per_chunk, per_chunk), per_chunk)
        return pltpu.make_async_copy(sources[6].at[at], members.at[at], sems.at[6 + c])

    small = [pltpu.make_async_copy(sources[i], held[i], sems.at[i]) for i in range(6)]
    for copy in small:
        copy.start()
    for c in range(chunks):
        fetch(c).start()

    def clear(t, _):
        total[t] = jnp.zeros(total.shape[1:], F32)
        return 0

    lax.fori_loop(0, total.shape[0], clear, 0, unroll=4)
    for copy in small:
        copy.wait()
    lane = iota((1, rows), 1)
    tail_row = iota((16, rows), 0)
    in_first = iota((size, LANES), 1) < size
    tail_first = in_first[:8] & (iota((8, LANES), 0) == 0)
    tail_second = ~in_first[:8] & (iota((8, LANES), 0) == 1)

    def scaled(n):
        perts = members[n].astype(F32)
        mean = jnp.sum(perts, axis=0, keepdims=True) / size
        root = jnp.sqrt(jnp.where(lane < count[n], weight[pl.ds(n, 1), :], 0.0))
        return ((perts - mean) * root).astype(BF16), (values[pl.ds(n, 1), :] - mean) * root

    def add_pair(i):
        one, innov_one = scaled(2 * i)
        two, innov_two = scaled(2 * i + 1)
        tail = jnp.where(tail_row == 0, innov_one, jnp.where(tail_row == 1, innov_two, 0.0))
        right = jnp.concatenate([one, two], axis=0)
        left = jnp.concatenate([one, two, tail.astype(BF16)], axis=0)
        products = lax.dot_general(
            left, right, (((1,), (1,)), ((), ())), preferred_element_type=F32
        )
        ends = products[2 * size : 2 * size + 8]
        t = target_of(tile[2 * i], block[2 * i], turn[2 * i])
        total[t, :size] = total[t, :size] + jnp.where(in_first, products[:size], 0.0)
        total[t, size:] = total[t, size:] + jnp.where(tail_first, ends, 0.0)
        t = target_of(tile[2 * i + 1], block[2 * i + 1], turn[2 * i + 1])
        total[t, :size] = total[t, :size] + jnp.where(in_first, 0.0, products[size : 2 * size])
        total[t, size:] = total[t, size:] + jnp.where(tail_second, ends, 0.0)
        return 0

    def add_chunk(c, _):
        fetch(c).wait()
        half_chunk = per_chunk // 2

        def step(i, _):
            return add_pair(c * half_chunk + i)

        return lax.fori_loop(0, half_chunk, step, 0, unroll=4)

    lax.fori_loop(0, chunks, add_chunk, 0)

    half = size // 2
    lane_half = iota((half, LANES), 1)
    col = lane_half % size
    row = iota((half, LANES), 0)
    from_top = (col >= half) | (col <= row)
    on_diag = col == row
    core = lax.axis_index("core")
    row8 = iota((8, LANES), 0)

    def halves_added(even, odd, mask):
        one = jnp.where(mask, even, odd)
        two = jnp.where(mask, odd, even)
        return one, pltpu.roll(two, size, 1)

    def pack(d, side):
        base = d * (CORES * own) + side * own
        bodies = []
        tail = jnp.zeros((8, LANES), F32)
        for pair in range(own // 2):
            even, odd = base + 2 * pair, base + 2 * pair + 1
            both = sum(halves_added(total[even, :size], total[odd, :size], in_first))
            top = both[:half]
            bottom = pltpu.roll(both[half:size], LANES - half, 1)
            bodies.append(jnp.where(from_top, top, bottom))
            diag = jnp.sum(jnp.where(on_diag, bottom, 0.0), axis=0, keepdims=True)
            one, two = halves_added(total[even, size:], total[odd, size:], in_first[:8])
            projections = jnp.sum(one + two, axis=0, keepdims=True)
            tail = jnp.where(row8 == 2 * pair, projections, tail)
            tail = jnp.where(row8 == 2 * pair + 1, diag, tail)
        return jnp.concatenate(bodies + [tail], axis=0)

    def pack_both(d, _):
        keep[d] = pack(d, core)
        send[d] = pack(d, 1 - core).astype(BF16)
        return 0

    lax.fori_loop(0, send.shape[0], pack_both, 0)


def hbm():
    return pl.BlockSpec(memory_space=pltpu.HBM)


def params(mib):
    return pltpu.CompilerParams(vmem_limit_bytes=mib * 1024 * 1024)


def scaled_grams(own, count, tile, block, turn, values, weight, members, tiles):
    blocks, size, rows = members.shape
    dests = tiles * ABLK // (CORES * own)
    shape = (dests, packed_rows(own), LANES)
    chunks = 4
    small = tiles * ABLK * (size + 8) * LANES * 4 // (1024 * 1024)
    return pl.pallas_call(
        functools.partial(gram_kernel, own, chunks),
        out_shape=(jax.ShapeDtypeStruct(shape, BF16), jax.ShapeDtypeStruct(shape, F32)),
        in_specs=[hbm()] * 7,
        out_specs=(whole(), whole()),
        scratch_shapes=[pltpu.SMEM((blocks,), jnp.int32)] * 4
        + [pltpu.VMEM((blocks, rows), F32)] * 2
        + [
            pltpu.VMEM((blocks, size, rows), BF16),
            pltpu.VMEM((tiles * ABLK, size + 8, LANES), F32),
            pltpu.SemaphoreType.DMA((6 + chunks,)),
        ],
        compiler_params=params(small + 12),
        name="grams",
    )(count, tile, block, turn, values, weight, members)


def split(x):
    high = x.astype(BF16)
    return high, (x - high.astype(F32)).astype(BF16)


def left_of(x, first_half):
    high, low = split(x)
    return jnp.concatenate([high, jnp.where(first_half, low, jnp.zeros_like(low))], axis=1)


def right_of(x):
    high, low = split(x)
    return jnp.concatenate([high, low, high, high], axis=0)


def times(left, right):
    return jnp.dot(left, right, preferred_element_type=F32)


def transform_kernel(own, size, groups, arrived, weights_out, *rest):
    outs, spread = rest[:groups], rest[groups]
    summed = arrived[0].astype(F32)
    for s in range(1, arrived.shape[0]):
        summed = summed + arrived[s].astype(F32)
    half = size // 2
    col = iota((half, LANES), 1) % size
    row = iota((half, LANES), 0)
    upper = col >= half
    eye = (iota((size, LANES), 1) % size == iota((size, LANES), 0)).astype(F32)
    first_half = iota((size, LANES), 1) < size
    extra = 16 * own
    systems, projections = [], []
    for pair in range(own // 2):
        part = summed[half * pair : half * (pair + 1)]
        projection = summed[extra + 2 * pair : extra + 2 * pair + 1]
        diag = pltpu.roll(summed[extra : extra + 8], half, 1)[2 * pair + 1 : 2 * pair + 2]
        low = jnp.where(col < row, part, jnp.where(col == row, 0.5 * part, 0.0))
        top = jnp.where(upper, part, low)
        moved = pltpu.roll(part, half, 1)
        high = jnp.where(
            col - half > row, moved, jnp.where(col - half == row, 0.5 * diag, 0.0)
        )
        bottom = jnp.where(upper, high, 0.0)
        fold = jnp.concatenate([top, bottom], axis=0)
        turned = fold.T
        other = pltpu.roll(fold, size, 1)
        for t in range(2):
            here = turned[size * t : size * (t + 1)]
            here = jnp.concatenate([here, here], axis=1)
            one, two = (fold, other) if t == 0 else (other, fold)
            gram = jnp.where(first_half, one, two) + here
            systems.append((size - 1.0) * eye + gram)
            shifted = projection if t == 0 else pltpu.roll(
                jnp.broadcast_to(projection, (8, LANES)), size, 1
            )[:1]
            projections.append(shifted)
    inverse_frobs, roots, inverses = [], [], []
    for system in systems:
        squares = jnp.where(first_half, system * system, 0.0)
        frob = jnp.sqrt(jnp.sum(jnp.sum(squares, axis=0, keepdims=True), axis=1, keepdims=True))
        inverse_frobs.append(frob)
        roots.append(system / frob)
    for step in range(NS_STEPS):
        if step == 0:
            middles = [1.5 * eye - 0.5 * s for s in roots]
        else:
            middles = [
                1.5 * eye - 0.5 * times(left_of(z, first_half), right_of(s))
                for z, s in zip(inverses, roots)
            ]
        if step == 0:
            roots = [times(left_of(s, first_half), right_of(e)) for s, e in zip(roots, middles)]
            inverses = middles
        elif step < NS_STEPS - 1:
            stacked = [
                times(
                    jnp.concatenate([left_of(s, first_half), left_of(z, first_half)], axis=0),
                    right_of(e),
                )
                for s, z, e in zip(roots, inverses, middles)
            ]
            roots = [x[:size] for x in stacked]
            inverses = [x[size:] for x in stacked]
        else:
            inverses = [
                times(left_of(z, first_half), right_of(e)) for z, e in zip(inverses, middles)
            ]
    share = size // groups
    me = lax.axis_index("y") * CORES + lax.axis_index("core")
    rows8 = iota((8, LANES), 0)
    weights = jnp.zeros((8, LANES), F32)
    for q in range(own):
        inverse_root = inverses[q] / jnp.sqrt(inverse_frobs[q])
        spread[q] = jnp.sqrt(size - 1.0) * inverse_root
        moved = jnp.sum(
            jnp.where(first_half, inverse_root * projections[q], 0.0), axis=1, keepdims=True
        )
        mean_weights = jnp.sum(inverse_root * moved, axis=0, keepdims=True)
        weights = jnp.where(rows8 == q, mean_weights, weights)
    weights_out[...] = weights
    for b in range(groups):
        start = pl.multiple_of((me ^ b) * share, share)
        for q in range(own):
            outs[b][pl.ds(q * share, share), :] = spread[q, pl.ds(start, share), :].astype(BF16)


def transforms(own, size, groups, arrived):
    share = size // groups
    return pl.pallas_call(
        functools.partial(transform_kernel, own, size, groups),
        out_shape=(jax.ShapeDtypeStruct((8, LANES), F32),)
        + tuple(jax.ShapeDtypeStruct((own * share, LANES), BF16) for _ in range(groups)),
        in_specs=[whole()],
        out_specs=tuple([whole()] * (groups + 1)),
        scratch_shapes=[pltpu.VMEM((own, size, LANES), F32)],
        compiler_params=params(8),
        name="transforms",
    )(arrived)


def centre_kernel(*refs):
    groups = len(refs) - 2
    parts, pert, mean_out = refs[:groups], refs[groups], refs[groups + 1]
    share, ablk, width = parts[0].shape
    size = share * groups
    step = 256

    def one(c, _):
        at = pl.ds(pl.multiple_of(c * step, step), step)
        total = jnp.zeros((ablk, step), F32)
        for part in parts:
            for i in range(share):
                total = total + part[i, :, at].astype(F32)
        mean = total / size
        mean_out[:, at] = mean
        for b, part in enumerate(parts):
            for i in range(share):
                pert[pl.ds((b * share + i) * ablk, ablk), at] = (
                    part[i, :, at].astype(F32) - mean
                ).astype(BF16)
        return 0

    lax.fori_loop(0, width // step, one, 0)


def centred(parts):
    share, ablk, width = parts[0].shape
    return pl.pallas_call(
        centre_kernel,
        out_shape=(
            jax.ShapeDtypeStruct((len(parts) * share * ablk, width), BF16),
            jax.ShapeDtypeStruct((ablk, width), F32),
        ),
        in_specs=[whole()] * len(parts),
        out_specs=(whole(), whole()),
        compiler_params=params(12),
        name="centre",
    )(*parts)


def apply_kernel(own, groups, weights, pert, mean, *refs):
    arrived, out_pert, out_mean, staged, sems = refs[:groups], *refs[groups:]
    size_by_block, width = pert.shape
    share = arrived[0].shape[0] // own
    rows = share * ABLK
    me = lax.axis_index("y") * CORES + lax.axis_index("core")
    received = jnp.concatenate([r[...] for r in arrived], axis=0)
    per_source = own * share
    count = groups * per_source
    to_row = iota((rows, count), 0)
    from_row = iota((rows, count), 1)
    source = me ^ (from_row // per_source)
    within = from_row % per_source
    place = (to_row // ABLK == within % share) & (
        to_row % ABLK == source * own + within // share
    )
    spread = times(place.astype(F32).astype(BF16), received).astype(BF16)
    spread = jnp.concatenate([spread, weights[...].astype(BF16), jnp.zeros((8, LANES), BF16)], axis=0)
    column = iota((LANES, size_by_block), 1)
    member = (me ^ (column // (share * ABLK))) * share + (column // ABLK) % share
    repeat = (iota((LANES, size_by_block), 0) == member).astype(F32).astype(BF16)
    wide = times(spread, repeat)
    wide_row = iota(wide.shape, 0)
    block = jnp.where(wide_row < rows, wide_row % ABLK, me * own + wide_row - rows)
    wide = jnp.where(block == iota(wide.shape, 1) % ABLK, wide, 0.0).astype(BF16)
    step = staged.shape[2]
    copies = []
    for c in range(width // step):
        at = pl.ds(c * step, step)
        result = times(wide, pert[:, at])
        staged[c] = result[:rows].astype(BF16)
        copies.append(pltpu.make_async_copy(staged.at[c], out_pert.at[:, at], sems.at[c]))
        copies[-1].start()
        means = mean[:, at]
        own_mean = means[:own]
        for m in range(1, groups):
            own_mean = jnp.where(me == m, means[m * own : (m + 1) * own], own_mean)
        out_mean[:, at] = (own_mean + result[rows : rows + own]).astype(BF16)
    for copy in copies:
        copy.wait()


def applied(own, weights, pert, mean, arrived):
    groups = len(arrived)
    share = arrived[0].shape[0] // own
    width = pert.shape[1]
    step = 256
    return pl.pallas_call(
        functools.partial(apply_kernel, own, groups),
        out_shape=(
            jax.ShapeDtypeStruct((share * ABLK, width), BF16),
            jax.ShapeDtypeStruct((own, width), BF16),
        ),
        in_specs=[whole()] * (3 + groups),
        out_specs=(hbm(), whole()),
        scratch_shapes=[
            pltpu.VMEM((width // step, share * ABLK, step), BF16),
            pltpu.SemaphoreType.DMA((width // step,)),
        ],
        compiler_params=params(16),
        name="apply",
    )(weights, pert, mean, *arrived)


def body(ensemble, obs_members, obs_values, obs_weight, obs_count, obs_tile, obs_block, obs_turn):
    tiles = lax.axis_size("tile")
    groups = lax.axis_size("y") * CORES
    own = ABLK // groups
    size = obs_members.shape[1]
    across = [(i, i ^ 1) for i in range(CORES)]

    def swapped(x, b):
        pairs = [(i, i ^ b) for i in range(groups)]
        return lax.ppermute(x, ("y", "core"), pairs)

    far = [swapped(ensemble, b) for b in range(2, groups, 2)]
    near = swapped(ensemble, 1)
    send, keep = scaled_grams(
        own, obs_count, obs_tile, obs_block, obs_turn, obs_values, obs_weight,
        obs_members, tiles,
    )
    got = lax.ppermute(send, "core", across)
    mine = (keep + got.astype(F32)).astype(BF16)
    arrived = lax.all_to_all(mine, ("tile", "y"), split_axis=0, concat_axis=0, tiled=True)
    parts = [ensemble, near]
    for x in far:
        parts += [x, lax.ppermute(x, "core", across)]
    pert, mean = centred(parts)
    weights, *spreads = transforms(own, size, groups, arrived)
    spreads = [spreads[0]] + [swapped(s, b) for b, s in enumerate(spreads) if b]
    analysis_pert, analysis_mean = applied(own, weights, pert, mean, spreads)
    return analysis_pert.reshape(ensemble.shape), analysis_mean


def solution(mesh):
    tiles, groups = mesh.shape["tile"], mesh.shape["mem"]
    fine = Mesh(mesh.devices.reshape(tiles, groups // CORES, CORES), ("tile", "y", "core"))
    everyone = ("tile", "y", "core")
    placed = (
        P(("y", "core"), "tile", None),
        P(everyone, None, None),
        P(everyone, None),
        P(everyone, None),
        P(everyone),
        P(everyone),
        P(everyone),
        P(everyone),
    )
    return jax.shard_map(
        body,
        mesh=fine,
        in_specs=placed,
        out_specs=(P(("y", "core"), "tile", None), P(everyone, None)),
        check_vma=False,
    )
```

```python
import functools

import jax
import jax.numpy as jnp
from jax import lax
from jax.experimental import pallas as pl
from jax.experimental.pallas import tpu as pltpu
from jax.sharding import Mesh, PartitionSpec as P


BPS = 4
ABLK = BPS * BPS
NS_STEPS = 6
CORES = 2
LANES = 128
F32 = jnp.float32
BF16 = jnp.bfloat16


def iota(shape, dim):
    return lax.broadcasted_iota(jnp.int32, shape, dim)


def my_group():
    return (lax.axis_index("yhi") * 2 + lax.axis_index("ylo")) * CORES + lax.axis_index("core")


def packed_rows(own):
    return (16 * own + own + 7) // 8 * 8


def whole():
    return pl.BlockSpec(memory_space=pltpu.VMEM)


def target_of(tile, block, turn):
    row, col = block >> 2, block & 3
    last = BPS - 1
    new_row = jnp.where(
        turn == 0, row, jnp.where(turn == 1, col, jnp.where(turn == 2, last - row, last - col))
    )
    new_col = jnp.where(
        turn == 0, col, jnp.where(turn == 1, last - row, jnp.where(turn == 2, last - col, row))
    )
    return tile * ABLK + new_row * BPS + new_col


def gram_kernel(own, chunks, *refs):
    sources, (send, total) = refs[:7], refs[7:9]
    held, sems = refs[9:16], refs[16]
    count, tile, block, turn, values, weight, members = held
    blocks, size, rows = members.shape
    per_chunk = blocks // chunks

    def fetch(c):
        at = pl.ds(pl.multiple_of(c * per_chunk, per_chunk), per_chunk)
        return pltpu.make_async_copy(sources[6].at[at], members.at[at], sems.at[6 + c])

    small = [pltpu.make_async_copy(sources[i], held[i], sems.at[i]) for i in range(6)]
    for copy in small:
        copy.start()
    for c in range(chunks):
        fetch(c).start()

    def clear(t, _):
        total[t] = jnp.zeros(total.shape[1:], F32)
        return 0

    lax.fori_loop(0, total.shape[0], clear, 0, unroll=4)
    for copy in small:
        copy.wait()
    lane = iota((1, rows), 1)
    tail_row = iota((16, rows), 0)
    in_first = iota((size, LANES), 1) < size
    tail_first = in_first[:8] & (iota((8, LANES), 0) == 0)
    tail_second = ~in_first[:8] & (iota((8, LANES), 0) == 1)

    def scaled(n):
        perts = members[n].astype(F32)
        mean = jnp.sum(perts, axis=0, keepdims=True) / size
        root = jnp.sqrt(jnp.where(lane < count[n], weight[pl.ds(n, 1), :], 0.0))
        return ((perts - mean) * root).astype(BF16), (values[pl.ds(n, 1), :] - mean) * root

    def add_pair(i):
        one, innov_one = scaled(2 * i)
        two, innov_two = scaled(2 * i + 1)
        tail = jnp.where(tail_row == 0, innov_one, jnp.where(tail_row == 1, innov_two, 0.0))
        right = jnp.concatenate([one, two], axis=0)
        left = jnp.concatenate([one, two, tail.astype(BF16)], axis=0)
        products = lax.dot_general(
            left, right, (((1,), (1,)), ((), ())), preferred_element_type=F32
        )
        ends = products[2 * size : 2 * size + 8]
        t = target_of(tile[2 * i], block[2 * i], turn[2 * i])
        total[t, :size] = total[t, :size] + jnp.where(in_first, products[:size], 0.0)
        total[t, size:] = total[t, size:] + jnp.where(tail_first, ends, 0.0)
        t = target_of(tile[2 * i + 1], block[2 * i + 1], turn[2 * i + 1])
        total[t, :size] = total[t, :size] + jnp.where(in_first, 0.0, products[size : 2 * size])
        total[t, size:] = total[t, size:] + jnp.where(tail_second, ends, 0.0)
        return 0

    def add_chunk(c, _):
        fetch(c).wait()
        half_chunk = per_chunk // 2

        def step(i, _):
            return add_pair(c * half_chunk + i)

        return lax.fori_loop(0, half_chunk, step, 0, unroll=16)

    lax.fori_loop(0, chunks, add_chunk, 0)

    pack_side(own, size, total, send, 1 - lax.axis_index("core"))


def pack_side(own, size, total, out, side):
    half = size // 2
    col = iota((half, LANES), 1) % size
    row = iota((half, LANES), 0)
    from_top = (col >= half) | (col <= row)
    on_diag = col == row
    in_first = iota((size, LANES), 1) < size
    row8 = iota((8, LANES), 0)

    def halves_added(even, odd, mask):
        one = jnp.where(mask, even, odd)
        two = jnp.where(mask, odd, even)
        return one + pltpu.roll(two, size, 1)

    def pack(d, _):
        base = d * (CORES * own) + side * own
        tail = jnp.zeros((8, LANES), F32)
        for pair in range(own // 2):
            even, odd = base + 2 * pair, base + 2 * pair + 1
            both = halves_added(total[even, :size], total[odd, :size], in_first)
            top = both[:half]
            bottom = pltpu.roll(both[half:size], LANES - half, 1)
            folded = jnp.where(from_top, top, bottom)
            out[d, half * pair : half * (pair + 1)] = folded.astype(out.dtype)
            diag = jnp.sum(jnp.where(on_diag, bottom, 0.0), axis=0, keepdims=True)
            ends = halves_added(total[even, size:], total[odd, size:], in_first[:8])
            tail = jnp.where(row8 == 2 * pair, jnp.sum(ends, axis=0, keepdims=True), tail)
            tail = jnp.where(row8 == 2 * pair + 1, diag, tail)
        out[d, 16 * own :] = tail.astype(out.dtype)
        return 0

    lax.fori_loop(0, out.shape[0], pack, 0, unroll=2)


def keep_kernel(own, size, total, keep):
    pack_side(own, size, total, keep, lax.axis_index("core"))


def kept(own, size, total):
    dests = total.shape[0] // (CORES * own)
    return pl.pallas_call(
        functools.partial(keep_kernel, own, size),
        out_shape=jax.ShapeDtypeStruct((dests, packed_rows(own), LANES), F32),
        in_specs=[whole()],
        out_specs=whole(),
        compiler_params=params(total.size * 4 // (1024 * 1024) + 8),
        name="keep",
    )(total)


def plane_kernel(highs, keep, got, mine, *outs):
    rows_high = highs[1]
    tlo, ylo = lax.axis_index("tlo"), lax.axis_index("ylo")

    def one(slot, _):
        for r in range(4):
            tile = (slot // rows_high) * 2 + (tlo ^ (r // 2))
            row = (slot % rows_high) * 2 + (ylo ^ (r % 2))
            d = tile * (2 * rows_high) + row
            both = keep[d] + got[d].astype(F32)
            if r == 0:
                mine[slot] = both
            else:
                outs[r - 1][slot] = both.astype(BF16)
        return 0

    lax.fori_loop(0, mine.shape[0], one, 0)


def plane_parts(highs, keep, got):
    slots = highs[0] * highs[1]
    shape = (slots,) + keep.shape[1:]
    return pl.pallas_call(
        functools.partial(plane_kernel, highs),
        out_shape=(jax.ShapeDtypeStruct(shape, F32),) + (jax.ShapeDtypeStruct(shape, BF16),) * 3,
        in_specs=[whole()] * 2,
        out_specs=(whole(),) * 4,
        compiler_params=params(12),
        name="plane",
    )(keep, got)


def line_kernel(stacked, *refs):
    mine, got, outs = refs[0], refs[1:4], refs[4:]
    z = lax.axis_index("thi") if not stacked else 0
    for s in range(mine.shape[0]):
        at = s if stacked else z ^ s
        total = mine[at] + sum(g[at].astype(F32) for g in got)
        if stacked:
            outs[0][s] = total.astype(BF16)
        else:
            outs[s][...] = total.astype(outs[s].dtype)


def line_parts(stacked, mine, got):
    slots, one = mine.shape[0], mine.shape[1:]
    if stacked:
        shapes = (jax.ShapeDtypeStruct(mine.shape, BF16),)
    else:
        shapes = (jax.ShapeDtypeStruct(one, F32),) + (jax.ShapeDtypeStruct(one, BF16),) * (slots - 1)
    return pl.pallas_call(
        functools.partial(line_kernel, stacked),
        out_shape=shapes,
        in_specs=[whole()] * 4,
        out_specs=(whole(),) * len(shapes),
        compiler_params=params(12),
        name="line",
    )(mine, *got)


def hbm():
    return pl.BlockSpec(memory_space=pltpu.HBM)


def stay(x):
    return pltpu.with_memory_space_constraint(x, pltpu.HBM)


def params(mib):
    return pltpu.CompilerParams(vmem_limit_bytes=mib * 1024 * 1024)


def scaled_grams(own, count, tile, block, turn, values, weight, members, tiles):
    blocks, size, rows = members.shape
    dests = tiles * ABLK // (CORES * own)
    shape = (dests, packed_rows(own), LANES)
    chunks = 4
    sums = (tiles * ABLK, size + 8, LANES)
    mib = tiles * ABLK * (size + 8) * LANES * 4 // (1024 * 1024)
    return pl.pallas_call(
        functools.partial(gram_kernel, own, chunks),
        out_shape=(jax.ShapeDtypeStruct(shape, BF16), jax.ShapeDtypeStruct(sums, F32)),
        in_specs=[hbm()] * 7,
        out_specs=(whole(), whole()),
        scratch_shapes=[pltpu.SMEM((blocks,), jnp.int32)] * 4
        + [pltpu.VMEM((blocks, rows), F32)] * 2
        + [
            pltpu.VMEM((blocks, size, rows), BF16),
            pltpu.SemaphoreType.DMA((6 + chunks,)),
        ],
        compiler_params=params(mib + 12),
        name="grams",
    )(*(stay(x) for x in (count, tile, block, turn, values, weight, members)))


def split(x):
    high = x.astype(BF16)
    return high, (x - high.astype(F32)).astype(BF16)


def left_of(x, first_half):
    high, low = split(x)
    return jnp.concatenate([high, jnp.where(first_half, low, jnp.zeros_like(low))], axis=1)


def right_of(x):
    high, low = split(x)
    return jnp.concatenate([high, low, high, high], axis=0)


def times(left, right):
    return jnp.dot(left, right, preferred_element_type=F32)


def transform_kernel(own, size, groups, *refs):
    outs, spread, weights_out = refs[-groups - 1 : -1], refs[-1], refs[-groups - 2]
    pieces = []
    for ref in refs[: -groups - 2]:
        pieces += [ref[...]] if len(ref.shape) == 2 else [ref[i] for i in range(ref.shape[0])]
    summed = sum(piece.astype(F32) for piece in pieces)
    half = size // 2
    col = iota((half, LANES), 1) % size
    row = iota((half, LANES), 0)
    upper = col >= half
    eye = (iota((size, LANES), 1) % size == iota((size, LANES), 0)).astype(F32)
    first_half = iota((size, LANES), 1) < size
    extra = 16 * own
    systems, projections = [], []
    for pair in range(own // 2):
        part = summed[half * pair : half * (pair + 1)]
        projection = summed[extra + 2 * pair : extra + 2 * pair + 1]
        diag = pltpu.roll(summed[extra : extra + 8], half, 1)[2 * pair + 1 : 2 * pair + 2]
        low = jnp.where(col < row, part, jnp.where(col == row, 0.5 * part, 0.0))
        top = jnp.where(upper, part, low)
        moved = pltpu.roll(part, half, 1)
        high = jnp.where(
            col - half > row, moved, jnp.where(col - half == row, 0.5 * diag, 0.0)
        )
        bottom = jnp.where(upper, high, 0.0)
        fold = jnp.concatenate([top, bottom], axis=0)
        turned = fold.T
        other = pltpu.roll(fold, size, 1)
        for t in range(2):
            here = turned[size * t : size * (t + 1)]
            here = jnp.concatenate([here, here], axis=1)
            one, two = (fold, other) if t == 0 else (other, fold)
            gram = jnp.where(first_half, one, two) + here
            systems.append((size - 1.0) * eye + gram)
            shifted = projection if t == 0 else pltpu.roll(
                jnp.broadcast_to(projection, (8, LANES)), size, 1
            )[:1]
            projections.append(shifted)
    inverse_frobs, roots, inverses = [], [], []
    for system in systems:
        squares = jnp.where(first_half, system * system, 0.0)
        frob = jnp.sqrt(jnp.sum(jnp.sum(squares, axis=0, keepdims=True), axis=1, keepdims=True))
        inverse_frobs.append(frob)
        roots.append(system / frob)
    for step in range(NS_STEPS):
        if step == 0:
            middles = [1.5 * eye - 0.5 * s for s in roots]
        else:
            middles = [
                1.5 * eye - 0.5 * times(left_of(z, first_half), right_of(s))
                for z, s in zip(inverses, roots)
            ]
        if step == 0:
            roots = [times(left_of(s, first_half), right_of(e)) for s, e in zip(roots, middles)]
            inverses = middles
        elif step < NS_STEPS - 1:
            stacked = [
                times(
                    jnp.concatenate([left_of(s, first_half), left_of(z, first_half)], axis=0),
                    right_of(e),
                )
                for s, z, e in zip(roots, inverses, middles)
            ]
            roots = [x[:size] for x in stacked]
            inverses = [x[size:] for x in stacked]
        else:
            inverses = [
                times(left_of(z, first_half), right_of(e)) for z, e in zip(inverses, middles)
            ]
    share = size // groups
    me = my_group()
    rows8 = iota((8, LANES), 0)
    weights = jnp.zeros((8, LANES), F32)
    for q in range(own):
        inverse_root = inverses[q] / jnp.sqrt(inverse_frobs[q])
        spread[q] = jnp.sqrt(size - 1.0) * inverse_root
        moved = jnp.sum(
            jnp.where(first_half, inverse_root * projections[q], 0.0), axis=1, keepdims=True
        )
        mean_weights = jnp.sum(inverse_root * moved, axis=0, keepdims=True)
        weights = jnp.where(rows8 == q, mean_weights, weights)
    weights_out[...] = weights
    for b in range(groups):
        start = pl.multiple_of((me ^ b) * share, share)
        for q in range(own):
            outs[b][pl.ds(q * share, share), :] = spread[q, pl.ds(start, share), :].astype(BF16)


def transforms(own, size, groups, arrived):
    share = size // groups
    return pl.pallas_call(
        functools.partial(transform_kernel, own, size, groups),
        out_shape=(jax.ShapeDtypeStruct((8, LANES), F32),)
        + tuple(jax.ShapeDtypeStruct((own * share, LANES), BF16) for _ in range(groups)),
        in_specs=[whole()] * len(arrived),
        out_specs=tuple([whole()] * (groups + 1)),
        scratch_shapes=[pltpu.VMEM((own, size, LANES), F32)],
        compiler_params=params(8),
        name="transforms",
    )(*arrived)


def centre_kernel(*refs):
    groups = len(refs) - 2
    parts, pert, mean_out = refs[:groups], refs[groups], refs[groups + 1]
    share, ablk, width = parts[0].shape
    size = share * groups
    step = 256

    def one(c, _):
        at = pl.ds(pl.multiple_of(c * step, step), step)
        total = jnp.zeros((ablk, step), F32)
        for part in parts:
            for i in range(share):
                total = total + part[i, :, at].astype(F32)
        mean = total / size
        mean_out[:, at] = mean
        for b, part in enumerate(parts):
            for i in range(share):
                pert[pl.ds((b * share + i) * ablk, ablk), at] = (
                    part[i, :, at].astype(F32) - mean
                ).astype(BF16)
        return 0

    lax.fori_loop(0, width // step, one, 0)


def centred(parts):
    share, ablk, width = parts[0].shape
    return pl.pallas_call(
        centre_kernel,
        out_shape=(
            jax.ShapeDtypeStruct((len(parts) * share * ablk, width), BF16),
            jax.ShapeDtypeStruct((ablk, width), F32),
        ),
        in_specs=[whole()] * len(parts),
        out_specs=(whole(), whole()),
        compiler_params=params(12),
        name="centre",
    )(*parts)


def apply_kernel(own, groups, weights, pert, mean, *refs):
    arrived, out_pert, out_mean, staged, sems = refs[:groups], *refs[groups:]
    size_by_block, width = pert.shape
    share = arrived[0].shape[0] // own
    rows = share * ABLK
    me = my_group()
    received = jnp.concatenate([r[...] for r in arrived], axis=0)
    per_source = own * share
    count = groups * per_source
    to_row = iota((rows, count), 0)
    from_row = iota((rows, count), 1)
    source = me ^ (from_row // per_source)
    within = from_row % per_source
    place = (to_row // ABLK == within % share) & (
        to_row % ABLK == source * own + within // share
    )
    spread = times(place.astype(F32).astype(BF16), received).astype(BF16)
    spread = jnp.concatenate([spread, weights[...].astype(BF16), jnp.zeros((8, LANES), BF16)], axis=0)
    column = iota((LANES, size_by_block), 1)
    member = (me ^ (column // (share * ABLK))) * share + (column // ABLK) % share
    repeat = (iota((LANES, size_by_block), 0) == member).astype(F32).astype(BF16)
    wide = times(spread, repeat)
    wide_row = iota(wide.shape, 0)
    block = jnp.where(wide_row < rows, wide_row % ABLK, me * own + wide_row - rows)
    wide = jnp.where(block == iota(wide.shape, 1) % ABLK, wide, 0.0).astype(BF16)
    step = staged.shape[2]
    copies = []
    for c in range(width // step):
        at = pl.ds(c * step, step)
        result = times(wide, pert[:, at])
        staged[c] = result[:rows].astype(BF16)
        copies.append(pltpu.make_async_copy(staged.at[c], out_pert.at[:, at], sems.at[c]))
        copies[-1].start()
        means = mean[:, at]
        own_mean = means[:own]
        for m in range(1, groups):
            own_mean = jnp.where(me == m, means[m * own : (m + 1) * own], own_mean)
        out_mean[:, at] = (own_mean + result[rows : rows + own]).astype(BF16)
    for copy in copies:
        copy.wait()


def applied(own, weights, pert, mean, arrived):
    groups = len(arrived)
    share = arrived[0].shape[0] // own
    width = pert.shape[1]
    step = 256
    return pl.pallas_call(
        functools.partial(apply_kernel, own, groups),
        out_shape=(
            jax.ShapeDtypeStruct((share * ABLK, width), BF16),
            jax.ShapeDtypeStruct((own, width), BF16),
        ),
        in_specs=[whole()] * (3 + groups),
        out_specs=(hbm(), whole()),
        scratch_shapes=[
            pltpu.VMEM((width // step, share * ABLK, step), BF16),
            pltpu.SemaphoreType.DMA((width // step,)),
        ],
        compiler_params=params(16),
        name="apply",
    )(weights, pert, mean, *arrived)


def body(ensemble, obs_members, obs_values, obs_weight, obs_count, obs_tile, obs_block, obs_turn):
    highs = (lax.axis_size("thi"), lax.axis_size("yhi"))
    tiles, groups = highs[0] * 2, highs[1] * 2 * CORES
    own = ABLK // groups
    size = obs_members.shape[1]
    across = [(i, i ^ 1) for i in range(CORES)]

    def swapped(x, b, axes, count):
        return lax.ppermute(x, axes, [(i, i ^ b) for i in range(count)])

    mem = ("yhi", "ylo", "core")
    far = [swapped(ensemble, b, mem, groups) for b in range(2, groups, 2)]
    near = swapped(ensemble, 1, mem, groups)
    send, total = scaled_grams(
        own, obs_count, obs_tile, obs_block, obs_turn, obs_values, obs_weight,
        obs_members, tiles,
    )
    got = lax.ppermute(send, "core", across)
    keep = kept(own, size, total)
    mine, *sends = plane_parts(highs, keep, got)
    got = []
    for r, x in enumerate(sends):
        got.append(swapped(x, r + 1, ("tlo", "ylo"), 4))
    stacked = highs[1] > 1 or highs[0] > 4
    arrived = list(line_parts(stacked, mine, got))
    if stacked:
        arrived = [
            lax.all_to_all(arrived[0], ("thi", "yhi"), split_axis=0, concat_axis=0, tiled=True)
        ]
    else:
        for s in range(1, highs[0]):
            arrived[s] = swapped(arrived[s], s, ("thi",), highs[0])
    parts = [ensemble, near]
    for x in far:
        parts += [x, lax.ppermute(x, "core", across)]
    pert, mean = centred(parts)
    weights, *spreads = transforms(own, size, groups, arrived)
    for b in range(1, groups):
        spreads[b] = swapped(spreads[b], b, mem, groups)
    analysis_pert, analysis_mean = applied(own, weights, pert, mean, spreads)
    return analysis_pert.reshape(ensemble.shape), analysis_mean


def solution(mesh):
    tiles, groups = mesh.shape["tile"], mesh.shape["mem"]
    shape = (tiles // 2, 2, groups // (2 * CORES), 2, CORES)
    fine = Mesh(mesh.devices.reshape(shape), ("thi", "tlo", "yhi", "ylo", "core"))
    tile, mem = ("thi", "tlo"), ("yhi", "ylo", "core")
    everyone = tile + mem
    placed = (
        P(mem, tile, None),
        P(everyone, None, None),
        P(everyone, None),
        P(everyone, None),
        P(everyone),
        P(everyone),
        P(everyone),
        P(everyone),
    )
    return jax.shard_map(
        body,
        mesh=fine,
        in_specs=placed,
        out_specs=(P(mem, tile, None), P(everyone, None)),
        check_vma=False,
    )
```
